256 devices in a mesh: dp: 8 (over x, y_lo), expert: 16 (over z, core), tensor: 2 (over y_hi).
Axes of the slice: x: 4, y: 4 (y_hi: 2, y_lo: 2; y = y_hi * 2 + y_lo), z: 8, core: 2. Of those that a mesh axis runs over, the one named last changes fastest.
Arguments:
- tokens: bfloat16 [1536, 256, 1280], P(('dp', 'expert', 'tensor')), may hold values from -16 to 16
- cotangent: bfloat16 [1536, 256, 1280], P(('dp', 'expert', 'tensor')), may hold values from -6 to 6
- norm_gain: float32 [1280], replicated, may hold values from 0.5 to 1.5
- slot_keys: bfloat16 [1280, 32], replicated, may hold values from -2 to 2
- w_in: bfloat16 [16, 1280, 2560], P('expert', None, 'tensor'), may hold values from -0.15625 to 0.15625
- w_out: bfloat16 [16, 2560, 1280], P('expert', 'tensor'), may hold values from -0.125 to 0.125
Outputs:
- grad_tokens: bfloat16 [1536, 256, 1280], P(('dp', 'expert', 'tensor'))
- grad_gain: float32 [1280], replicated
- grad_keys: float32 [1280, 32], replicated
- grad_in: bfloat16 [16, 1280, 2560], P('expert', 'dp', 'tensor')
- grad_out: bfloat16 [16, 2560, 1280], P('expert', 'tensor', 'dp')
The draws below stay inside these ranges and needn't reach their ends.
All inputs are finite; a program needn't handle non-finite values.
Results may differ from the reference program's by a relative error of at most 0.014.
The reference program's roundings to bfloat16 on the way count: a program that leaves them out, or rounds other values in their place, can miss the bound.
Values may be sent and summed in bfloat16 or wider, within the bound.
No kernel may reach another device: no remote copies, remote signals or barrier semaphores. Data moves between devices by JAX's collectives and lax.ppermute only.
A program may use at most 128 MiB of HBM per device.

```python
import math
import jax
import jax.numpy as jnp
from jax import lax

D = 1280
TOK_IMG = 256
SLOT_PER = 2
FF = 2560
IMG_DEV = 6
EXPERTS = 16
SLOTS = 32
IMAGES = 1536


def draw_slot_keys(key, part):
    values = jax.random.normal(jax.random.fold_in(key, 11), (D, SLOTS), jnp.float32) * (1.0 / math.sqrt(D))
    limit = 1.0 + 2000 // D
    return jnp.clip(values, -limit, limit).astype(jnp.bfloat16)


def draw_tokens(key, part):
    values = jax.random.normal(jax.random.fold_in(key, 21), (IMAGES, TOK_IMG, D), jnp.float32)
    return jnp.clip(values, -16.0, 16.0).astype(jnp.bfloat16)


def level_of(rng, shape, split, smallest, largest):
    factor_of = 1.0
    for dim, blocks in split:
        draws = jax.random.uniform(jax.random.fold_in(jax.random.fold_in(rng, 6), dim), (blocks,), jnp.float32, smallest / len(split), largest / len(split))
        factor_of = factor_of * jnp.repeat(jnp.exp(draws), shape[dim] // blocks).reshape((-1,) + (1,) * (len(shape) - 1 - dim))
    return factor_of


def bell_draw(rng, extent, scale, most, split=(), dtype=jnp.bfloat16):
    values = scale * jax.random.normal(rng, extent, jnp.float32)
    if split:
        values = values * level_of(rng, extent, split, -0.22, 0.18)
    return jnp.clip(values, -most, most).astype(dtype)


def setup_inputs(seed: int = 0) -> dict:
    arg_keys = jax.random.split(jax.random.key(seed), 7)
    tokens = draw_tokens(jax.random.fold_in(arg_keys[6], 71), 0)
    cotangent = bell_draw(arg_keys[1], (IMAGES, TOK_IMG, D), 1.0, 6.0, ((0, 256),))
    norm_gain = jnp.clip(1.0 + 0.1 * jax.random.normal(arg_keys[2], (D,), jnp.float32), 0.5, 1.5)
    slot_keys = draw_slot_keys(jax.random.fold_in(arg_keys[6], 71), 0)
    w_in = bell_draw(arg_keys[4], (EXPERTS, D, FF), D ** -0.5, 0.15625, ((0, 16), (2, 2)))
    w_out = bell_draw(arg_keys[5], (EXPERTS, FF, D), FF ** -0.5, 0.125, ((0, 16), (1, 2)))
    return dict(tokens=tokens, cotangent=cotangent, norm_gain=norm_gain, slot_keys=slot_keys, w_in=w_in, w_out=w_out)


EPSILON = 1e-06

def rounded(values):
    lowered = lax.optimization_barrier(values.astype(jnp.bfloat16))
    return values + lax.stop_gradient(lowered.astype(jnp.float32) - values)

def mixing(tokens_wide, gain, keys_wide):
    average = lax.optimization_barrier(jnp.mean(tokens_wide, axis=-1, keepdims=True))
    centred = tokens_wide - average
    spread = lax.optimization_barrier(jnp.mean(centred * centred, axis=-1, keepdims=True))
    normed = rounded(centred * lax.rsqrt(spread + EPSILON) * gain)
    logits = jnp.einsum('bmd,dn->bmn', normed, keys_wide, precision=lax.Precision.HIGHEST)
    dispatch = rounded(jax.nn.softmax(logits, axis=1))
    combine = jax.nn.softmax(logits, axis=2)
    slot_values = jnp.einsum('bmn,bmd->bnd', dispatch, normed, precision=lax.Precision.HIGHEST)
    return (slot_values, combine)

def expert_forward(slot_rows, first_proj, second_proj):
    pre_act = jnp.dot(slot_rows.astype(jnp.float32), first_proj.astype(jnp.float32), preferred_element_type=jnp.float32)
    hidden = jax.nn.gelu(pre_act).astype(jnp.bfloat16)
    return jnp.dot(hidden.astype(jnp.float32), second_proj.astype(jnp.float32), preferred_element_type=jnp.float32).astype(jnp.bfloat16)

def expert_backward(slot_rows, row_grads, first_proj, second_proj):
    pre_act = jnp.dot(slot_rows.astype(jnp.float32), first_proj.astype(jnp.float32), preferred_element_type=jnp.float32)
    hidden = jax.nn.gelu(pre_act).astype(jnp.bfloat16)
    grad_hidden = lax.dot_general(row_grads.astype(jnp.float32), second_proj.astype(jnp.float32), (((1,), (1,)), ((), ())), preferred_element_type=jnp.float32)
    grad_pre = jax.vjp(jax.nn.gelu, pre_act)[1](grad_hidden)[0].astype(jnp.bfloat16)
    grad_rows = lax.dot_general(grad_pre.astype(jnp.float32), first_proj.astype(jnp.float32), (((1,), (1,)), ((), ())), preferred_element_type=jnp.float32)
    grad_first = lax.dot_general(slot_rows.astype(jnp.float32), grad_pre.astype(jnp.float32), (((0,), (0,)), ((), ())), preferred_element_type=jnp.float32)
    grad_second = lax.dot_general(hidden.astype(jnp.float32), row_grads.astype(jnp.float32), (((0,), (0,)), ((), ())), preferred_element_type=jnp.float32)
    return (grad_rows.astype(jnp.bfloat16), grad_first.astype(jnp.bfloat16), grad_second.astype(jnp.bfloat16))

def to_experts(per_image, images):
    experts = SLOTS // SLOT_PER
    shaped = per_image.reshape(images, experts, SLOT_PER, D)
    return jnp.transpose(shaped, (1, 0, 2, 3)).reshape(experts, images * SLOT_PER, D)

def from_experts(per_expert, images):
    experts = SLOTS // SLOT_PER
    shaped = per_expert.reshape(experts, images, SLOT_PER, D)
    return jnp.transpose(shaped, (1, 0, 2, 3)).reshape(images // IMG_DEV, IMG_DEV, SLOTS, D)

def reference(tokens, cotangent, norm_gain, slot_keys, w_in, w_out):
    images = tokens.shape[0]
    groups = images // IMG_DEV
    image_blocks = tokens.reshape(groups, IMG_DEV, TOK_IMG, D)
    grad_blocks = cotangent.reshape(groups, IMG_DEV, TOK_IMG, D)
    keys_wide = slot_keys.astype(jnp.float32)

    def forward_block(image_block):
        slot_values, combine = mixing(image_block.astype(jnp.float32), norm_gain, keys_wide)
        return (slot_values.astype(jnp.bfloat16), combine.astype(jnp.bfloat16))
    slot_inputs, combine_low = lax.map(forward_block, image_blocks)
    expert_rows = to_experts(slot_inputs, images)
    slot_outputs = lax.map(lambda inputs: expert_forward(inputs[0], inputs[1], inputs[2]), (expert_rows, w_in, w_out))
    slot_outputs = from_experts(slot_outputs, images)

    def combine_block(inputs):
        comb_block, grad_block, out_block = inputs
        grad_slots = jnp.einsum('bmn,bmd->bnd', comb_block.astype(jnp.float32), grad_block.astype(jnp.float32))
        grad_combine = jnp.einsum('bmd,bnd->bmn', grad_block.astype(jnp.float32), out_block.astype(jnp.float32))
        return (grad_slots.astype(jnp.bfloat16), grad_combine)
    grad_slots, grad_combine = lax.map(combine_block, (combine_low, grad_blocks, slot_outputs))
    grad_rows_in = to_experts(grad_slots, images)
    grad_rows, grad_first, grad_second = lax.map(lambda inputs: expert_backward(inputs[0], inputs[1], inputs[2], inputs[3]), (expert_rows, grad_rows_in, w_in, w_out))
    grad_slot_in = from_experts(grad_rows, images)

    def mixing_back(totals, inputs):
        image_block, grad_block, slot_grad, comb_grad = inputs
        unused, pullback = jax.vjp(mixing, image_block.astype(jnp.float32), norm_gain, keys_wide)
        grad_tok, grad_gain, grad_keys = pullback((slot_grad.astype(jnp.float32), comb_grad))
        result = (grad_block.astype(jnp.float32) + grad_tok).astype(jnp.bfloat16)
        return ((totals[0] + grad_gain, totals[1] + grad_keys), result)
    start_totals = (jnp.zeros((D,), jnp.float32), jnp.zeros((D, SLOTS), jnp.float32))
    totals, grad_tokens = lax.scan(mixing_back, start_totals, (image_blocks, grad_blocks, grad_slot_in, grad_combine))
    return (grad_tokens.reshape(images, TOK_IMG, D), totals[0], totals[1], grad_first, grad_second)
```

```python
import jax
import jax.numpy as jnp
from jax import lax
from jax.sharding import PartitionSpec as P

SLOT_PER = 2


EPSILON = 1e-06

ROWS = 24
LANES = 128


def from_everyone(shard, axis):
    devices = lax.axis_size(axis)
    return lax.all_to_all(
        jnp.broadcast_to(shard[None], (devices, *shard.shape)), axis, 0, 0, tiled=True
    )


def swapped(value):
    return lax.ppermute(value, "tensor", [(0, 1), (1, 0)])


def mixing_forward(tokens, gain, slot_keys):
    average = jnp.mean(tokens, axis=-1, keepdims=True, dtype=jnp.float32)
    centred = tokens.astype(jnp.float32) - average
    spread = jnp.mean(centred * centred, axis=-1, keepdims=True)
    inverse = lax.rsqrt(spread + EPSILON)
    scaled = centred * inverse
    normed = (scaled * gain).astype(jnp.bfloat16)
    logits = jnp.einsum("bmd,dn->bmn", normed, slot_keys, preferred_element_type=jnp.float32)
    dispatch = jax.nn.softmax(logits, axis=1)
    combine = jax.nn.softmax(logits, axis=2)
    dispatch_low = dispatch.astype(jnp.bfloat16)
    slot_values = jnp.einsum(
        "bmn,bmd->bnd", dispatch_low, normed, preferred_element_type=jnp.float32
    )
    return (slot_values, combine, (scaled, inverse, normed, dispatch, combine, dispatch_low))


def split_wide(value):
    high = value.astype(jnp.bfloat16)
    low = (value - high.astype(jnp.float32)).astype(jnp.bfloat16)
    return high, low


def contract_rows(left, right):
    return lax.dot_general(
        left, right, (((0,), (0,)), ((), ())), preferred_element_type=jnp.float32
    )


def contract_cols(left, right):
    return lax.dot_general(
        left, right, (((1,), (1,)), ((), ())), preferred_element_type=jnp.float32
    )


def summed_everywhere(keys_term, gain_part):
    slots, features = keys_term.shape
    blocks = features // LANES
    group = lax.axis_size("expert")
    flat = jnp.concatenate(
        [
            keys_term.reshape(slots, blocks, LANES).transpose(1, 0, 2).reshape(-1, LANES),
            gain_part.reshape(blocks, LANES),
            jnp.zeros((group * ROWS - (slots + 1) * blocks, LANES), jnp.float32),
        ]
    ).reshape(group, ROWS, LANES)
    mine = jnp.sum(lax.all_to_all(flat, "expert", 0, 0, tiled=True), axis=0)
    mine = jnp.sum(from_everyone(mine, ("dp", "tensor")), axis=0)
    whole = from_everyone(mine, "expert").reshape(-1, LANES)
    keys_sum = whole[: slots * blocks].reshape(blocks, slots, LANES).transpose(1, 0, 2)
    return keys_sum.reshape(slots, features), whole[slots * blocks :][:blocks].reshape(-1)


def local(tokens, cotangent, norm_gain, slot_keys, w_in, w_out):
    local_imgs, token_count, features = tokens.shape
    slot_count = slot_keys.shape[1]
    experts = slot_count // SLOT_PER
    slot_values, combine, saved = mixing_forward(tokens, norm_gain, slot_keys)
    slot_low = slot_values.astype(jnp.bfloat16)
    slot_inputs = slot_low.reshape(local_imgs, experts, SLOT_PER, features)
    arrived = lax.all_to_all(slot_inputs, "expert", split_axis=1, concat_axis=0, tiled=True)
    own = arrived.reshape(-1, features)
    half = own.shape[0]
    slot_rows = jnp.concatenate([own, swapped(own)])
    combine_low = combine.astype(jnp.bfloat16)
    grad_slots = jnp.einsum(
        "bmn,bmd->bnd", combine_low, cotangent, preferred_element_type=jnp.float32
    )
    grad_slots = grad_slots.astype(jnp.bfloat16).reshape(local_imgs, experts, SLOT_PER, features)
    grads_sent = lax.all_to_all(grad_slots, "expert", split_axis=1, concat_axis=0, tiled=True)
    own_grads = grads_sent.reshape(-1, features)
    grad_rows = jnp.concatenate([own_grads, swapped(own_grads)])
    first_proj = w_in[0]
    second_proj = w_out[0]
    pre_act = jnp.dot(slot_rows, first_proj, preferred_element_type=jnp.float32)
    hidden = jax.nn.gelu(pre_act).astype(jnp.bfloat16)

    def reduced_and_returned(partial):
        theirs = swapped(partial[half:].astype(jnp.bfloat16))
        total = (partial[:half] + theirs.astype(jnp.float32)).astype(jnp.bfloat16)
        return lax.all_to_all(
            total.reshape(arrived.shape), "expert", split_axis=0, concat_axis=1, tiled=True
        ).reshape(local_imgs, slot_count, features)

    returned = reduced_and_returned(jnp.dot(hidden, second_proj, preferred_element_type=jnp.float32))
    grad_hidden = contract_cols(grad_rows, second_proj)
    grad_pre = jax.vjp(jax.nn.gelu, pre_act)[1](grad_hidden)[0].astype(jnp.bfloat16)
    grad_back = reduced_and_returned(contract_cols(grad_pre, first_proj))
    second_part = contract_rows(grad_rows, hidden).astype(jnp.bfloat16)
    first_part = contract_rows(slot_rows, grad_pre).astype(jnp.bfloat16)
    grad_second = lax.psum_scatter(second_part, "dp", scatter_dimension=0, tiled=True)
    grad_first = lax.psum_scatter(first_part, "dp", scatter_dimension=0, tiled=True)
    returned, grad_back, second_part, first_part = lax.optimization_barrier(
        (returned, grad_back, second_part, first_part)
    )

    scaled, inverse, normed, dispatch, combine, dispatch_low = saved
    combine_grad = jnp.einsum(
        "bmd,bnd->bmn", cotangent, returned, preferred_element_type=jnp.float32
    )
    grad_dispatch = jnp.einsum(
        "bnd,bmd->bmn", grad_back, normed, preferred_element_type=jnp.float32
    )
    grad_logits = dispatch * (
        grad_dispatch - jnp.sum(dispatch * grad_dispatch, axis=1, keepdims=True)
    )
    grad_logits = grad_logits + combine * (
        combine_grad - jnp.sum(combine * combine_grad, axis=2, keepdims=True)
    )
    high, low = split_wide(grad_logits)
    pair = jnp.concatenate([high, low], axis=2)
    keys_pair = jnp.einsum("bmn,bmd->nd", pair, normed, preferred_element_type=jnp.float32)
    keys_term = keys_pair[:slot_count] + keys_pair[slot_count:]
    gain_part = jnp.sum(grad_back.astype(jnp.float32) * slot_low.astype(jnp.float32), axis=(0, 1))
    keys_sum, gain_sum = summed_everywhere(keys_term, gain_part)
    keys_wide = slot_keys.astype(jnp.float32)
    grad_keys = keys_sum.T
    grad_gain = (gain_sum + jnp.sum(keys_wide * grad_keys, axis=1)) / norm_gain

    weights = jnp.concatenate([dispatch_low, pair], axis=2)
    keys_rows = jnp.broadcast_to(slot_keys.T[None], (local_imgs, slot_count, features))
    values = jnp.concatenate([grad_back, keys_rows, keys_rows], axis=1)
    grad_normed = jnp.einsum("bmn,bnd->bmd", weights, values, preferred_element_type=jnp.float32)
    grad_scaled = grad_normed * norm_gain
    first_mean = jnp.mean(grad_scaled, axis=-1, keepdims=True)
    second_mean = jnp.mean(grad_scaled * scaled, axis=-1, keepdims=True)
    grad_tok = inverse * (grad_scaled - first_mean - scaled * second_mean)
    grad_tokens = (cotangent.astype(jnp.float32) + grad_tok).astype(jnp.bfloat16)
    return (
        grad_tokens,
        grad_gain,
        grad_keys,
        grad_first[None],
        grad_second.T[None],
    )


def solution(mesh):
    placed = (
        P(("dp", "expert", "tensor"), None, None),
        P(("dp", "expert", "tensor"), None, None),
        P(),
        P(),
        P("expert", None, "tensor"),
        P("expert", "tensor", None),
    )
    return jax.shard_map(
        local,
        mesh=mesh,
        in_specs=placed,
        out_specs=(
            P(("dp", "expert", "tensor"), None, None),
            P(),
            P(),
            P("expert", "dp", "tensor"),
            P("expert", "tensor", "dp"),
        ),
        check_vma=False,
    )
```

```python
import jax
import jax.numpy as jnp
from jax import lax
from jax.experimental import pallas as pl
from jax.experimental.pallas import tpu as pltpu
from jax.sharding import PartitionSpec as P


SLOT_PER = 2


EPSILON = 1e-06


ROWS = 24
LANES = 128
CHUNK = 16
MIB = 1024 * 1024


def dot(left, right, dims):
    return lax.dot_general(left, right, (dims, ((), ())), preferred_element_type=jnp.float32)


NN = ((1,), (0,))
NT = ((1,), (1,))
TN = ((0,), (0,))


def from_everyone(shard, axis):
    devices = lax.axis_size(axis)
    return lax.all_to_all(
        jnp.broadcast_to(shard[None], (devices, *shard.shape)), axis, 0, 0, tiled=True
    )


def swapped(value):
    return lax.ppermute(value, "tensor", [(0, 1), (1, 0)])


def call(kernel, outs, ins, args, grid=None, scratch=(), flops=0, moved=0, limit=None):
    specs = {} if grid is None else {"grid": (grid,)}
    return pl.pallas_call(
        kernel,
        out_shape=[jax.ShapeDtypeStruct(s, d) for s, d, _ in outs],
        in_specs=list(ins),
        out_specs=[spec for _, _, spec in outs],
        scratch_shapes=list(scratch),
        compiler_params=pltpu.CompilerParams(vmem_limit_bytes=limit),
        cost_estimate=pl.CostEstimate(flops=flops, bytes_accessed=moved, transcendentals=0),
        **specs,
    )(*args)


def per_image(rows, cols):
    return pl.BlockSpec((1, rows, cols), lambda i: (i, 0, 0))


def whole(*shape):
    return pl.BlockSpec(shape, lambda i: (0,) * len(shape))


def packed_place(place, images):
    block = images * SLOT_PER
    place = place.astype(jnp.float32)
    expert = jnp.floor((place + 0.5) * (1.0 / (2 * block)))
    rest = place - expert * (2 * block)
    half = jnp.floor((rest + 0.5) * (1.0 / block))
    rest = rest - half * block
    image = jnp.floor((rest + 0.5) * (1.0 / SLOT_PER))
    return expert, half, image, rest - image * SLOT_PER


def selection(rows, images, half, by_image, packed_first):
    shape = (2 * rows, rows) if packed_first else (rows, 2 * rows)
    along = 0 if packed_first else 1
    thin = (2 * rows, 1) if packed_first else (1, 2 * rows)
    expert, part, image, slot = packed_place(lax.broadcasted_iota(jnp.int32, thin, along), images)
    if by_image:
        target = image * (rows // images) + expert * SLOT_PER + slot
    else:
        target = expert * (images * SLOT_PER) + image * SLOT_PER + slot
    target = jnp.where(part == half, target, -1.0)
    plain = lax.broadcasted_iota(jnp.int32, shape, 1 - along).astype(jnp.float32)
    return jnp.where(plain == target, 1.0, 0.0).astype(jnp.bfloat16)


def pack(value, images, by_image):
    rows, cols = value.shape
    total = 0.0
    for half in range(2):
        pick = selection(rows, images, half, by_image, True)
        total = total + dot(pick, value[:, half * (cols // 2) : (half + 1) * (cols // 2)], NN)
    return total.astype(jnp.bfloat16)


def unpack_into(out_ref, value, images, by_image):
    rows, cols = out_ref.shape
    for half in range(2):
        pick = selection(rows, images, half, by_image, False)
        out_ref[:, half * (cols // 2) : (half + 1) * (cols // 2)] = dot(pick, value, NN).astype(
            jnp.bfloat16
        )


def parts(wide, count):
    pieces = []
    for _ in range(count):
        piece = wide.astype(jnp.bfloat16)
        pieces.append(piece)
        wide = wide - piece.astype(jnp.float32)
    return pieces


def over_chunks(count, body):
    def group(g, carry):
        for part in range(4):
            body(pl.ds(pl.multiple_of((g * 4 + part) * CHUNK, CHUNK), CHUNK))
        return carry

    lax.fori_loop(0, count // (4 * CHUNK), group, 0)


def lane_blocks(features):
    return [slice(k * LANES, (k + 1) * LANES) for k in range(features // LANES)]


def softmax(logits, axis):
    exps = jnp.exp(logits - jnp.max(logits, axis=axis, keepdims=True))
    return exps / jnp.sum(exps, axis=axis, keepdims=True)


def started(copies):
    for copy in copies:
        copy.start()
    return copies


def copies_of(sources, targets, sems):
    return [
        pltpu.make_async_copy(source, target, sems.at[i])
        for i, (source, target) in enumerate(zip(sources, targets))
    ]


def forward_kernel(images, *refs):
    inputs, outputs, held = refs[:3], refs[3:10], refs[10:]
    tok, gain, keys, send, slots, normed, inverse, logs, disp, comb, mean, squares = held[:12]
    in_sems, small_sems, exit_sems, out_sems = held[12:]
    count, features = tok.shape[1:]
    slot_count = keys.shape[0]
    tokens_in = [inputs[0].at[i] for i in range(images)]
    arrivals = started(copies_of(tokens_in, [tok.at[i] for i in range(images)], in_sems))
    small_in = started(copies_of(inputs[1:], [gain, keys], small_sems))
    exits = copies_of(
        [normed.at[i] for i in range(images)], [outputs[2].at[i] for i in range(images)], exit_sems
    )
    results = copies_of(
        [send, slots, inverse, logs, disp, comb], outputs[:2] + outputs[3:], out_sems
    )
    ones = jnp.ones((features, LANES), jnp.bfloat16)
    for i in range(images):
        arrivals[i].wait()
        mean[i] = dot(tok[i], ones, NN) * (1.0 / features)

        def square(rows):
            middle = mean[i, rows, :]
            total = jnp.zeros_like(middle)
            for at in lane_blocks(features):
                centred = tok[i, rows, at].astype(jnp.float32) - middle
                total = total + centred * centred
            squares[i, rows, :] = total

        over_chunks(count, square)
    for i in range(images):
        spread = 0.0
        for piece in parts(squares[i], 3):
            spread = spread + dot(piece, ones[:LANES], NN)
        inverse[i] = lax.rsqrt(spread * (1.0 / features) + EPSILON)
    results[2].start()
    for copy in small_in:
        copy.wait()
    for i in range(images):

        def norm(rows):
            middle = mean[i, rows, :]
            scale = inverse[i, rows, :]
            for at in lane_blocks(features):
                centred = tok[i, rows, at].astype(jnp.float32) - middle
                normed[i, rows, at] = (centred * scale * gain[0:1, at]).astype(jnp.bfloat16)

        over_chunks(count, norm)
        exits[i].start()
        logs[i] = dot(keys[...], normed[i], NT)
    results[3].start()
    for i in range(images):
        disp[i] = softmax(logs[i], 1)
        comb[i] = softmax(logs[i], 0)
    results[4].start()
    results[5].start()
    for i in range(images):
        values = dot(disp[i].astype(jnp.bfloat16), normed[i], NN)
        slots[i * slot_count : (i + 1) * slot_count, :] = values.astype(jnp.bfloat16)
    results[1].start()
    send[...] = pack(slots[...], images, True)
    results[0].start()
    for copy in exits + results:
        copy.wait()


def grads_kernel(images, cot, comb, send, slots):
    i = pl.program_id(0)
    count = comb.shape[1]
    values = dot(comb[0].astype(jnp.bfloat16), cot[0], NN)
    slots[pl.ds(pl.multiple_of(i * count, count), count), :] = values.astype(jnp.bfloat16)

    @pl.when(i == images - 1)
    def _():
        send[...] = pack(slots[...], images, True)


def unpack_kernel(images, value, out):
    unpack_into(out, value[...], images, False)


def add_pack_kernel(images, own, other, out):
    total = (own[...] + other[...].astype(jnp.float32)).astype(jnp.bfloat16)
    out[...] = pack(total, images, False)


def combine_kernel(images, far_back, hbm, far_comb, out, back, cot, comb, slots, sems, small_sems):
    smalls = started(copies_of([far_back, far_comb], [back, comb], small_sems))
    per = [hbm.at[i] for i in range(images)]
    arrivals = started(copies_of(per, [cot.at[i] for i in range(images)], sems))
    for copy in smalls:
        copy.wait()
    unpack_into(slots, back[...], images, True)
    count = comb.shape[1]
    for i in range(images):
        arrivals[i].wait()
        grad = dot(slots[i * count : (i + 1) * count, :], cot[i], NT)
        weight = comb[i]
        out[i] = weight * (grad - jnp.sum(weight * grad, axis=0, keepdims=True))


def logits_kernel(images, *refs):
    inputs, (grads, pair, sums), held = refs[:8], refs[8:11], refs[11:]
    back, slots, normed, logs, disp, part, keys, gain, total, sems, small_sems = held
    targets = [back, logs, disp, part, keys, gain, slots]
    sources = [inputs[0]] + list(inputs[3:]) + [inputs[1]]
    smalls = started(copies_of(sources, targets, small_sems))
    per = [inputs[2].at[i] for i in range(images)]
    arrivals = started(copies_of(per, [normed.at[i] for i in range(images)], sems))
    smalls[0].wait()
    unpack_into(grads, back[...], images, True)
    for copy in smalls[1:]:
        copy.wait()
    count = disp.shape[1]
    tokens = normed.shape[1]
    share = 1.0 / normed.shape[2]
    keys_share = jnp.sum(keys[...].astype(jnp.float32) * gain[...], axis=1, keepdims=True)
    place = lax.broadcasted_iota(jnp.int32, (16, tokens), 0)
    for i in range(images):
        arrivals[i].wait()
        mine = grads[i * count : (i + 1) * count, :]
        grad = dot(mine, normed[i], NT)
        weight = disp[i]
        wide = weight * (grad - jnp.sum(weight * grad, axis=1, keepdims=True)) + part[i]
        high, rest = parts(wide, 2)
        pair[i, :count, :] = high
        pair[i, count : 2 * count, :] = rest
        update = dot(pair[i, : 2 * count, :], normed[i], NN)
        total[...] = update if i == 0 else total[...] + update
        used = high.astype(jnp.float32) + rest.astype(jnp.float32)
        spread = weight.astype(jnp.bfloat16).astype(jnp.float32)
        mine_share = jnp.sum(mine.astype(jnp.float32) * gain[...], axis=1, keepdims=True)
        first = jnp.sum(spread * mine_share + used * keys_share, axis=0, keepdims=True) * share
        second = jnp.sum(spread * grad + used * logs[i], axis=0, keepdims=True) * share
        rows = jnp.zeros((16, tokens), jnp.float32)
        for k, row in enumerate(parts(first, 2) + parts(second, 2)):
            rows = jnp.where(place == k, row.astype(jnp.float32), rows)
        pair[i, 2 * count :, :] = rows.astype(jnp.bfloat16)
    product = grads[...].astype(jnp.float32) * slots[...].astype(jnp.float32)
    moved = jnp.sum(product, axis=0, keepdims=True)
    blocks = moved.shape[1] // LANES
    sums[blocks * count :, :] = jnp.zeros((sums.shape[0] - blocks * count, LANES), jnp.float32)
    for k, at in enumerate(lane_blocks(moved.shape[1])):
        sums[k * count : (k + 1) * count, :] = total[:count, at] + total[count:, at]
        sums[blocks * count + k : blocks * count + k + 1, :] = moved[:, at]


def tokens_kernel(normed, cot, inverse, pair, disp, grads, keys, gain, out, wide, inside):
    count, features = normed.shape[1:]
    weights = jnp.concatenate([disp[0].astype(jnp.bfloat16), pair[0]], axis=0)
    extra = weights.shape[0] - 3 * keys.shape[0]
    values = jnp.concatenate(
        [grads[...], keys[...], keys[...], jnp.zeros((extra, features), jnp.bfloat16)], axis=0
    )
    inside[...] = 1.0 / gain[...]
    wide[:, :features] = dot(weights, values, TN)
    row = lax.broadcasted_iota(jnp.int32, (extra, 2 * LANES), 0)
    col = lax.broadcasted_iota(jnp.int32, (extra, 2 * LANES), 1)
    pick = jnp.where((row < 4) & ((row < 2) == (col < LANES)), 1.0, 0.0).astype(jnp.bfloat16)
    wide[:, features:] = dot(pair[0, 2 * keys.shape[0] :, :], pick, TN)

    def norm(rows):
        first = wide[rows, features : features + LANES]
        second = wide[rows, features + LANES :]
        scale = inverse[0, rows, :]
        for at in lane_blocks(features):
            scaled = normed[0, rows, at].astype(jnp.float32) * inside[:, at]
            result = scale * (wide[rows, at] * gain[:, at] - first - scaled * second)
            out[0, rows, at] = (cot[0, rows, at].astype(jnp.float32) + result).astype(jnp.bfloat16)

    over_chunks(count, norm)


def after(value, *others):
    return lax.optimization_barrier((value, others))[0]


def piece_of(pieces, index, axis=0):
    return lax.dynamic_index_in_dim(pieces, index, axis, keepdims=False)


def chip_pairs(step, size):
    return [(i, (i + 2 * step) % size) for i in range(size)]


def to_other_chips(pieces):
    size = lax.axis_size("dp")
    chips = size // 2
    at = lax.axis_index("dp") // 2
    arrived = [
        lax.ppermute(piece_of(pieces, (at + step) % chips), "dp", chip_pairs(step, size))
        for step in range(1, chips)
    ]
    return [piece_of(pieces, at)] + arrived


def to_neighbour(value):
    return lax.ppermute(value, "dp", [(i, i ^ 1) for i in range(lax.axis_size("dp"))])


def added(pieces):
    total = pieces[0].astype(jnp.float32)
    for piece in pieces[1:]:
        total = total + piece.astype(jnp.float32)
    return total


def local(tokens, cotangent, norm_gain, slot_keys, w_in, w_out):
    images, count, features = tokens.shape
    slot_count = slot_keys.shape[1]
    rows = images * slot_count
    group = slot_count // SLOT_PER
    half = features // 2
    bf16, f32 = jnp.bfloat16, jnp.float32
    keys = slot_keys.T
    gain = norm_gain.reshape(1, features)
    tall = per_image(count, features)
    thin = per_image(slot_count, count)
    packed = whole(2 * rows, half)
    small = 2 * rows * features * count

    def sent(value):
        shaped = value.reshape(group, -1, half)
        return lax.all_to_all(shaped, "expert", 0, 0, tiled=True).reshape(2 * rows, half)

    local_ref = pl.BlockSpec(memory_space=pltpu.VMEM)
    far_ref = pl.BlockSpec(memory_space=pl.ANY)
    stacked = pltpu.VMEM((images, count, features), bf16)
    kept = [
        ((2 * rows, half), bf16),
        ((rows, features), bf16),
        ((images, count, features), bf16),
        ((images, count, LANES), f32),
        ((images, slot_count, count), f32),
        ((images, slot_count, count), f32),
        ((images, slot_count, count), f32),
    ]
    send_slots, slots, normed, inverse, logits, dispatch, combine = call(
        lambda *refs: forward_kernel(images, *refs),
        [(shape, kind, far_ref) for shape, kind in kept],
        [far_ref] * 3,
        (tokens, gain, keys),
        scratch=[stacked, pltpu.VMEM((1, features), f32), pltpu.VMEM((slot_count, features), bf16)]
        + [pltpu.VMEM(shape, kind) for shape, kind in kept]
        + [pltpu.VMEM((images, count, LANES), f32)] * 2
        + [pltpu.SemaphoreType.DMA((n,)) for n in (images, 2, images, 6)],
        flops=20 * small,
        moved=4 * images * count * features,
    )
    (send_grads,) = call(
        lambda *refs: grads_kernel(images, *refs),
        [((2 * rows, half), bf16, packed)],
        [tall, thin],
        (cotangent, combine),
        grid=images,
        scratch=[pltpu.VMEM((rows, features), bf16)],
        flops=10 * small,
        moved=2 * images * count * features,
    )

    def unpacked(value):
        return call(
            lambda *refs: unpack_kernel(images, *refs),
            [((rows, features), bf16, pl.BlockSpec(memory_space=pltpu.VMEM))],
            [pl.BlockSpec(memory_space=pltpu.VMEM)],
            (value,),
            flops=4 * small,
            moved=4 * rows * features,
            limit=16 * MIB,
        )[0]

    def summed(own, other):
        return call(
            lambda *refs: add_pack_kernel(images, *refs),
            [((2 * rows, half), bf16, pl.BlockSpec(memory_space=pltpu.VMEM))],
            [pl.BlockSpec(memory_space=pltpu.VMEM)] * 2,
            (own, other),
            flops=4 * small,
            moved=8 * rows * features,
            limit=16 * MIB,
        )[0]

    arrived = sent(send_slots)
    own_rows = unpacked(arrived)
    their_rows = swapped(own_rows)
    arrived = sent(send_grads)
    own_grads = unpacked(arrived)
    their_grads = swapped(own_grads)
    first_proj = w_in[0]
    second_proj = w_out[0]
    own_pre = dot(own_rows, first_proj, NN)
    own_hidden = jax.nn.gelu(own_pre).astype(bf16)
    their_pre = dot(their_rows, first_proj, NN)
    their_hidden = jax.nn.gelu(their_pre).astype(bf16)
    their_part = dot(their_hidden, second_proj, NN).astype(bf16)
    sums_out = swapped(their_part)

    def before_gelu(pre, grads):
        return jax.vjp(jax.nn.gelu, pre)[1](dot(grads, second_proj, NT))[0].astype(bf16)

    own_grad_pre = before_gelu(own_pre, own_grads)
    their_grad_pre = before_gelu(their_pre, their_grads)
    their_part = dot(their_grad_pre, first_proj, NT).astype(bf16)
    sums_in = swapped(their_part)
    own_part = dot(own_hidden, second_proj, NN)
    to_send = summed(own_part, sums_out)
    returned = sent(to_send)

    slot_rows = jnp.concatenate([own_rows, their_rows])
    grad_rows = jnp.concatenate([own_grads, their_grads])
    hidden = jnp.concatenate([own_hidden, their_hidden])
    grad_pre = jnp.concatenate([own_grad_pre, their_grad_pre])
    chips = lax.axis_size("dp") // 2
    low = lax.axis_index("dp") % 2
    second_part = dot(grad_rows, hidden, TN).astype(bf16).reshape(chips, -1, features)
    second_pieces = to_other_chips(second_part)
    first_part = dot(slot_rows, grad_pre, TN).astype(bf16).reshape(chips, 2, -1, features)
    own_part = dot(own_grad_pre, first_proj, NT)
    to_send = summed(own_part, sums_in)
    grad_back = sent(to_send)
    first_sent = after(piece_of(first_part, 1 - low, 1), sums_in)
    first_other = to_neighbour(first_sent)
    first_own = piece_of(first_part, low, 1)

    (combine_part,) = call(
        lambda *refs: combine_kernel(images, *refs),
        [((images, slot_count, count), f32, local_ref)],
        [far_ref] * 3,
        (returned, cotangent, combine),
        scratch=[
            pltpu.VMEM((2 * rows, half), bf16),
            stacked,
            pltpu.VMEM((images, slot_count, count), f32),
            pltpu.VMEM((rows, features), bf16),
            pltpu.SemaphoreType.DMA((images,)),
            pltpu.SemaphoreType.DMA((2,)),
        ],
        flops=10 * small,
        moved=2 * images * count * features,
    )
    grads, pair, sums = call(
        lambda *refs: logits_kernel(images, *refs),
        [
            ((rows, features), bf16, local_ref),
            ((images, 2 * slot_count + 16, count), bf16, local_ref),
            ((group * ROWS, LANES), f32, local_ref),
        ],
        [far_ref] * 8,
        (grad_back, slots, normed, logits, dispatch, combine_part, keys, gain),
        scratch=[
            pltpu.VMEM((2 * rows, half), bf16),
            pltpu.VMEM((rows, features), bf16),
            stacked,
        ]
        + [pltpu.VMEM((images, slot_count, count), f32)] * 3
        + [
            pltpu.VMEM((slot_count, features), bf16),
            pltpu.VMEM((1, features), f32),
            pltpu.VMEM((2 * slot_count, features), f32),
            pltpu.SemaphoreType.DMA((images,)),
            pltpu.SemaphoreType.DMA((7,)),
        ],
        flops=15 * small,
        moved=2 * images * count * features,
    )
    mine = lax.all_to_all(sums.reshape(group, ROWS, LANES), "expert", 0, 0, tiled=True)
    mine = jnp.sum(mine, axis=0)
    mine_two = from_everyone(mine, ("dp", "tensor"))
    first_other = after(first_other, mine)
    first_half = added([first_own, first_other]).astype(bf16)
    first_pieces = to_other_chips(first_half)
    second_pieces = after(second_pieces, mine)
    second_total = added(second_pieces).reshape(2, -1, features)
    second_other = to_neighbour(piece_of(second_total, 1 - low).astype(bf16))
    mine = jnp.sum(mine_two, axis=0)
    total = from_everyone(mine, "expert").reshape(-1, LANES)
    first_pieces = after(first_pieces, mine)
    grad_first = added(first_pieces).astype(bf16)
    second_other = after(second_other, mine)
    grad_second = added([piece_of(second_total, low), second_other]).astype(bf16)
    blocks = features // LANES
    keys_sum = total[: slot_count * blocks].reshape(blocks, slot_count, LANES)
    keys_sum = keys_sum.transpose(1, 0, 2).reshape(slot_count, features)
    gain_sum = total[slot_count * blocks :][:blocks].reshape(-1)
    gain_sum = gain_sum + jnp.sum(keys.astype(f32) * keys_sum, axis=0)

    (grad_tokens,) = call(
        tokens_kernel,
        [((images, count, features), bf16, tall)],
        [
            tall,
            tall,
            per_image(count, LANES),
            per_image(2 * slot_count + 16, count),
            thin,
            pl.BlockSpec((slot_count, features), lambda i: (i, 0)),
            whole(slot_count, features),
            whole(1, features),
        ],
        (normed, cotangent, inverse, pair, dispatch, grads, keys, gain),
        grid=images,
        scratch=[pltpu.VMEM((count, features + 2 * LANES), f32), pltpu.VMEM((1, features), f32)],
        flops=20 * small,
        moved=6 * images * count * features,
    )
    return (
        grad_tokens,
        gain_sum / norm_gain,
        keys_sum.T,
        grad_first[None],
        grad_second.T[None],
    )


def solution(mesh):
    placed = (
        P(("dp", "expert", "tensor"), None, None),
        P(("dp", "expert", "tensor"), None, None),
        P(),
        P(),
        P("expert", None, "tensor"),
        P("expert", "tensor", None),
    )
    return jax.shard_map(
        local,
        mesh=mesh,
        in_specs=placed,
        out_specs=(
            P(("dp", "expert", "tensor"), None, None),
            P(),
            P(),
            P("expert", "dp", "tensor"),
            P("expert", "tensor", "dp"),
        ),
        check_vma=False,
    )
```

```python
import jax
import jax.numpy as jnp
from jax import lax
from jax.experimental import pallas as pl
from jax.experimental.pallas import tpu as pltpu
from jax.sharding import PartitionSpec as P


SLOT_PER = 2


EPSILON = 1e-06


ROWS = 24
LANES = 128
CHUNK = 16
MIB = 1024 * 1024


def dot(left, right, dims):
    return lax.dot_general(left, right, (dims, ((), ())), preferred_element_type=jnp.float32)


NN = ((1,), (0,))
NT = ((1,), (1,))
TN = ((0,), (0,))


def from_everyone(shard, axis):
    devices = lax.axis_size(axis)
    return lax.all_to_all(
        jnp.broadcast_to(shard[None], (devices, *shard.shape)), axis, 0, 0, tiled=True
    )


def swapped(value):
    return lax.ppermute(value, "tensor", [(0, 1), (1, 0)])


def call(kernel, outs, ins, args, grid=None, scratch=(), flops=0, moved=0, limit=None):
    specs = {} if grid is None else {"grid": (grid,)}
    return pl.pallas_call(
        kernel,
        out_shape=[jax.ShapeDtypeStruct(s, d) for s, d, _ in outs],
        in_specs=list(ins),
        out_specs=[spec for _, _, spec in outs],
        scratch_shapes=list(scratch),
        compiler_params=pltpu.CompilerParams(vmem_limit_bytes=limit),
        cost_estimate=pl.CostEstimate(flops=flops, bytes_accessed=moved, transcendentals=0),
        **specs,
    )(*args)


def per_image(rows, cols):
    return pl.BlockSpec((1, rows, cols), lambda i: (i, 0, 0))


def whole(*shape):
    return pl.BlockSpec(shape, lambda i: (0,) * len(shape))


def packed_place(place, images):
    block = images * SLOT_PER
    place = place.astype(jnp.float32)
    expert = jnp.floor((place + 0.5) * (1.0 / (2 * block)))
    rest = place - expert * (2 * block)
    half = jnp.floor((rest + 0.5) * (1.0 / block))
    rest = rest - half * block
    image = jnp.floor((rest + 0.5) * (1.0 / SLOT_PER))
    return expert, half, image, rest - image * SLOT_PER


def selection(rows, images, half, by_image, packed_first):
    shape = (2 * rows, rows) if packed_first else (rows, 2 * rows)
    along = 0 if packed_first else 1
    thin = (2 * rows, 1) if packed_first else (1, 2 * rows)
    expert, part, image, slot = packed_place(lax.broadcasted_iota(jnp.int32, thin, along), images)
    if by_image:
        target = image * (rows // images) + expert * SLOT_PER + slot
    else:
        target = expert * (images * SLOT_PER) + image * SLOT_PER + slot
    target = jnp.where(part == half, target, -1.0)
    plain = lax.broadcasted_iota(jnp.int32, shape, 1 - along).astype(jnp.float32)
    return jnp.where(plain == target, 1.0, 0.0).astype(jnp.bfloat16)


def pack(value, images, by_image):
    rows, cols = value.shape
    total = 0.0
    for half in range(2):
        pick = selection(rows, images, half, by_image, True)
        total = total + dot(pick, value[:, half * (cols // 2) : (half + 1) * (cols // 2)], NN)
    return total.astype(jnp.bfloat16)


def unpack_into(out_ref, value, images, by_image):
    rows, cols = out_ref.shape
    for half in range(2):
        pick = selection(rows, images, half, by_image, False)
        out_ref[:, half * (cols // 2) : (half + 1) * (cols // 2)] = dot(pick, value, NN).astype(
            jnp.bfloat16
        )


def parts(wide, count):
    pieces = []
    for _ in range(count):
        piece = wide.astype(jnp.bfloat16)
        pieces.append(piece)
        wide = wide - piece.astype(jnp.float32)
    return pieces


def over_chunks(count, body):
    def group(g, carry):
        for part in range(4):
            body(pl.ds(pl.multiple_of((g * 4 + part) * CHUNK, CHUNK), CHUNK))
        return carry

    lax.fori_loop(0, count // (4 * CHUNK), group, 0)


def lane_blocks(features):
    return [slice(k * LANES, (k + 1) * LANES) for k in range(features // LANES)]


def softmax(logits, axis):
    exps = jnp.exp(logits - jnp.max(logits, axis=axis, keepdims=True))
    return exps / jnp.sum(exps, axis=axis, keepdims=True)


def started(copies):
    for copy in copies:
        copy.start()
    return copies


def copies_of(sources, targets, sems):
    return [
        pltpu.make_async_copy(source, target, sems.at[i])
        for i, (source, target) in enumerate(zip(sources, targets))
    ]


def forward_kernel(images, *refs):
    inputs, outputs, held = refs[:3], refs[3:10], refs[10:]
    tok, flat, keys, send, slots, normed, inverse, logs, disp, comb, mean, squares, gain = held[:13]
    in_sems, small_sems, exit_sems, out_sems = held[13:]
    count, features = tok.shape[1:]
    slot_count = keys.shape[0]
    tokens_in = [inputs[0].at[i] for i in range(images)]
    arrivals = started(copies_of(tokens_in, [tok.at[i] for i in range(images)], in_sems))
    small_in = started(copies_of(inputs[1:], [flat, keys], small_sems))
    exits = copies_of(
        [normed.at[i] for i in range(images)], [outputs[2].at[i] for i in range(images)], exit_sems
    )
    results = copies_of(
        [send, slots, inverse, logs, disp, comb], outputs[:2] + outputs[3:], out_sems
    )
    ones = jnp.ones((features, LANES), jnp.bfloat16)
    for i in range(images):
        arrivals[i].wait()
        mean[i] = dot(tok[i], ones, NN) * (1.0 / features)

        def square(rows):
            middle = mean[i, rows, :]
            total = jnp.zeros_like(middle)
            for at in lane_blocks(features):
                centred = tok[i, rows, at].astype(jnp.float32) - middle
                total = total + centred * centred
            squares[i, rows, :] = total

        over_chunks(count, square)
    for i in range(images):
        spread = 0.0
        for piece in parts(squares[i], 3):
            spread = spread + dot(piece, ones[:LANES], NN)
        inverse[i] = lax.rsqrt(spread * (1.0 / features) + EPSILON)
    results[2].start()
    for copy in small_in:
        copy.wait()
    gain[...] = flat[...].reshape(1, features)
    for i in range(images):

        def norm(rows):
            middle = mean[i, rows, :]
            scale = inverse[i, rows, :]
            for at in lane_blocks(features):
                centred = tok[i, rows, at].astype(jnp.float32) - middle
                normed[i, rows, at] = (centred * scale * gain[0:1, at]).astype(jnp.bfloat16)

        over_chunks(count, norm)
        exits[i].start()
        logs[i] = dot(keys[...], normed[i], NT)
    results[3].start()
    for i in range(images):
        disp[i] = softmax(logs[i], 1)
        comb[i] = softmax(logs[i], 0)
    results[4].start()
    results[5].start()
    for i in range(images):
        values = dot(disp[i].astype(jnp.bfloat16), normed[i], NN)
        slots[i * slot_count : (i + 1) * slot_count, :] = values.astype(jnp.bfloat16)
    results[1].start()
    send[...] = pack(slots[...], images, True)
    results[0].start()
    for copy in exits + results:
        copy.wait()


def grads_kernel(images, cot, comb, send, slots):
    i = pl.program_id(0)
    count = comb.shape[1]
    values = dot(comb[0].astype(jnp.bfloat16), cot[0], NN)
    slots[pl.ds(pl.multiple_of(i * count, count), count), :] = values.astype(jnp.bfloat16)

    @pl.when(i == images - 1)
    def _():
        send[...] = pack(slots[...], images, True)


def unpack_kernel(images, value, out):
    unpack_into(out, value[...], images, False)


def add_pack_kernel(images, own, other, out):
    total = (own[...] + other[...].astype(jnp.float32)).astype(jnp.bfloat16)
    out[...] = pack(total, images, False)


def combine_kernel(images, far_back, hbm, far_comb, out, back, cot, comb, slots, sems, small_sems):
    smalls = started(copies_of([far_back, far_comb], [back, comb], small_sems))
    per = [hbm.at[i] for i in range(images)]
    arrivals = started(copies_of(per, [cot.at[i] for i in range(images)], sems))
    for copy in smalls:
        copy.wait()
    unpack_into(slots, back[...], images, True)
    count = comb.shape[1]
    for i in range(images):
        arrivals[i].wait()
        grad = dot(slots[i * count : (i + 1) * count, :], cot[i], NT)
        weight = comb[i]
        out[i] = weight * (grad - jnp.sum(weight * grad, axis=0, keepdims=True))


def logits_kernel(images, *refs):
    inputs, (grads, pair, sums), held = refs[:8], refs[8:11], refs[11:]
    back, slots, normed, logs, disp, part, keys, gain, total, sems, small_sems = held
    targets = [back, logs, disp, part, keys, gain, slots]
    sources = [inputs[0]] + list(inputs[3:]) + [inputs[1]]
    smalls = started(copies_of(sources, targets, small_sems))
    per = [inputs[2].at[i] for i in range(images)]
    arrivals = started(copies_of(per, [normed.at[i] for i in range(images)], sems))
    smalls[0].wait()
    unpack_into(grads, back[...], images, True)
    for copy in smalls[1:]:
        copy.wait()
    count = disp.shape[1]
    tokens = normed.shape[1]
    share = 1.0 / normed.shape[2]
    keys_share = jnp.sum(keys[...].astype(jnp.float32) * gain[...], axis=1, keepdims=True)
    place = lax.broadcasted_iota(jnp.int32, (16, tokens), 0)
    for i in range(images):
        arrivals[i].wait()
        mine = grads[i * count : (i + 1) * count, :]
        grad = dot(mine, normed[i], NT)
        weight = disp[i]
        wide = weight * (grad - jnp.sum(weight * grad, axis=1, keepdims=True)) + part[i]
        high, rest = parts(wide, 2)
        pair[i, :count, :] = high
        pair[i, count : 2 * count, :] = rest
        update = dot(pair[i, : 2 * count, :], normed[i], NN)
        total[...] = update if i == 0 else total[...] + update
        used = high.astype(jnp.float32) + rest.astype(jnp.float32)
        spread = weight.astype(jnp.bfloat16).astype(jnp.float32)
        mine_share = jnp.sum(mine.astype(jnp.float32) * gain[...], axis=1, keepdims=True)
        first = jnp.sum(spread * mine_share + used * keys_share, axis=0, keepdims=True) * share
        second = jnp.sum(spread * grad + used * logs[i], axis=0, keepdims=True) * share
        rows = jnp.zeros((16, tokens), jnp.float32)
        for k, row in enumerate(parts(first, 2) + parts(second, 2)):
            rows = jnp.where(place == k, row.astype(jnp.float32), rows)
        pair[i, 2 * count :, :] = rows.astype(jnp.bfloat16)
    product = grads[...].astype(jnp.float32) * slots[...].astype(jnp.float32)
    moved = jnp.sum(product, axis=0, keepdims=True)
    blocks = moved.shape[1] // LANES
    sums[blocks * count :, :] = jnp.zeros((sums.shape[0] - blocks * count, LANES), jnp.float32)
    for k, at in enumerate(lane_blocks(moved.shape[1])):
        sums[k * count : (k + 1) * count, :] = total[:count, at] + total[count:, at]
        sums[blocks * count + k : blocks * count + k + 1, :] = moved[:, at]


def tokens_kernel(normed, cot, inverse, pair, disp, grads, keys, gain, out, wide, inside):
    count, features = normed.shape[1:]
    weights = jnp.concatenate([disp[0].astype(jnp.bfloat16), pair[0]], axis=0)
    extra = weights.shape[0] - 3 * keys.shape[0]
    values = jnp.concatenate(
        [grads[...], keys[...], keys[...], jnp.zeros((extra, features), jnp.bfloat16)], axis=0
    )
    inside[...] = 1.0 / gain[...]
    wide[:, :features] = dot(weights, values, TN)
    row = lax.broadcasted_iota(jnp.int32, (extra, 2 * LANES), 0)
    col = lax.broadcasted_iota(jnp.int32, (extra, 2 * LANES), 1)
    pick = jnp.where((row < 4) & ((row < 2) == (col < LANES)), 1.0, 0.0).astype(jnp.bfloat16)
    wide[:, features:] = dot(pair[0, 2 * keys.shape[0] :, :], pick, TN)

    def norm(rows):
        first = wide[rows, features : features + LANES]
        second = wide[rows, features + LANES :]
        scale = inverse[0, rows, :]
        for at in lane_blocks(features):
            scaled = normed[0, rows, at].astype(jnp.float32) * inside[:, at]
            result = scale * (wide[rows, at] * gain[:, at] - first - scaled * second)
            out[0, rows, at] = (cot[0, rows, at].astype(jnp.float32) + result).astype(jnp.bfloat16)

    over_chunks(count, norm)


def after(value, *others):
    return lax.optimization_barrier((value, others))[0]


def piece_of(pieces, index, axis=0):
    return lax.dynamic_index_in_dim(pieces, index, axis, keepdims=False)


def chip_pairs(step, size):
    return [(i, (i + 2 * step) % size) for i in range(size)]


def rotated_sum_kernel(where, far_part, far_other, *refs):
    chips = far_other.shape[0]
    outs, (part, other, sems) = refs[:chips], refs[chips:]
    order = [lax.rem(where[0] + k, chips) for k in range(chips)]
    copies = copies_of(
        [far_part.at[at, where[1]] for at in order] + [far_other.at[at] for at in order],
        [part.at[k] for k in range(chips)] + [other.at[k] for k in range(chips)],
        sems,
    )
    started(copies)
    for k in range(chips):
        copies[k].wait()
        copies[chips + k].wait()
        outs[k][...] = added([part[k], other[k]]).astype(jnp.bfloat16)


def rotated_sum(part, other):
    chips, _, rows, cols = part.shape
    index = lax.axis_index("dp")
    where = jnp.stack([index // 2, index % 2]).astype(jnp.int32)
    return call(
        rotated_sum_kernel,
        [((rows, cols), jnp.bfloat16, pl.BlockSpec(memory_space=pltpu.VMEM))] * chips,
        [pl.BlockSpec(memory_space=pltpu.SMEM)] + [pl.BlockSpec(memory_space=pl.ANY)] * 2,
        (where, part, other),
        scratch=[pltpu.VMEM((chips, rows, cols), jnp.bfloat16)] * 2
        + [pltpu.SemaphoreType.DMA((2 * chips,))],
        flops=100 * rows * cols * chips,
        moved=6 * rows * cols * chips,
    )


def split_sum_kernel(where, far_part, *refs):
    arrived, (kept, sent, held, sems) = refs[:-4], refs[-4:]
    chips = len(arrived) + 1
    rows = kept.shape[0]
    sources = [far_part.at[where[0]]] + list(arrived)
    copies = started(copies_of(sources, [held.at[k] for k in range(chips)], sems))
    for copy in copies:
        copy.wait()

    def total(low):
        at = pl.ds(pl.multiple_of(low * rows, CHUNK), rows)
        return added([held[k, at, :] for k in range(chips)])

    kept[...] = total(where[1])
    sent[...] = total(1 - where[1]).astype(jnp.bfloat16)


def split_sum(part, arrived):
    chips, rows, cols = part.shape
    index = lax.axis_index("dp")
    where = jnp.stack([index // 2, index % 2]).astype(jnp.int32)
    local_ref = pl.BlockSpec(memory_space=pltpu.VMEM)
    return call(
        split_sum_kernel,
        [((rows // 2, cols), jnp.float32, local_ref), ((rows // 2, cols), jnp.bfloat16, local_ref)],
        [pl.BlockSpec(memory_space=pltpu.SMEM)] + [pl.BlockSpec(memory_space=pl.ANY)] * chips,
        (where, part, *arrived),
        scratch=[pltpu.VMEM((chips, rows, cols), jnp.bfloat16), pltpu.SemaphoreType.DMA((chips,))],
        flops=100 * rows * cols * chips,
        moved=2 * rows * cols * chips,
    )


def to_other_chips(pieces):
    size = lax.axis_size("dp")
    chips = size // 2
    at = lax.axis_index("dp") // 2
    arrived = [
        lax.ppermute(piece_of(pieces, (at + step) % chips), "dp", chip_pairs(step, size))
        for step in range(1, chips)
    ]
    return arrived


def to_neighbour(value):
    return lax.ppermute(value, "dp", [(i, i ^ 1) for i in range(lax.axis_size("dp"))])


def added(pieces):
    total = pieces[0].astype(jnp.float32)
    for piece in pieces[1:]:
        total = total + piece.astype(jnp.float32)
    return total


def local(tokens, cotangent, norm_gain, slot_keys, w_in, w_out):
    images, count, features = tokens.shape
    slot_count = slot_keys.shape[1]
    rows = images * slot_count
    group = slot_count // SLOT_PER
    half = features // 2
    bf16, f32 = jnp.bfloat16, jnp.float32
    keys = slot_keys.T
    gain = norm_gain.reshape(1, features)
    tall = per_image(count, features)
    thin = per_image(slot_count, count)
    packed = whole(2 * rows, half)
    small = 2 * rows * features * count

    def sent(value):
        shaped = value.reshape(group, -1, half)
        return lax.all_to_all(shaped, "expert", 0, 0, tiled=True).reshape(2 * rows, half)

    local_ref = pl.BlockSpec(memory_space=pltpu.VMEM)
    far_ref = pl.BlockSpec(memory_space=pl.ANY)
    stacked = pltpu.VMEM((images, count, features), bf16)
    kept = [
        ((2 * rows, half), bf16),
        ((rows, features), bf16),
        ((images, count, features), bf16),
        ((images, count, LANES), f32),
        ((images, slot_count, count), f32),
        ((images, slot_count, count), f32),
        ((images, slot_count, count), f32),
    ]
    send_slots, slots, normed, inverse, logits, dispatch, combine = call(
        lambda *refs: forward_kernel(images, *refs),
        [(shape, kind, far_ref) for shape, kind in kept],
        [far_ref] * 3,
        (tokens, norm_gain, keys),
        scratch=[stacked, pltpu.VMEM((features,), f32), pltpu.VMEM((slot_count, features), bf16)]
        + [pltpu.VMEM(shape, kind) for shape, kind in kept]
        + [pltpu.VMEM((images, count, LANES), f32)] * 2
        + [pltpu.VMEM((1, features), f32)]
        + [pltpu.SemaphoreType.DMA((n,)) for n in (images, 2, images, 6)],
        flops=20 * small,
        moved=4 * images * count * features,
    )
    (send_grads,) = call(
        lambda *refs: grads_kernel(images, *refs),
        [((2 * rows, half), bf16, packed)],
        [tall, thin],
        (cotangent, combine),
        grid=images,
        scratch=[pltpu.VMEM((rows, features), bf16)],
        flops=10 * small,
        moved=2 * images * count * features,
    )

    def unpacked(value):
        return call(
            lambda *refs: unpack_kernel(images, *refs),
            [((rows, features), bf16, pl.BlockSpec(memory_space=pltpu.VMEM))],
            [pl.BlockSpec(memory_space=pltpu.VMEM)],
            (value,),
            flops=4 * small,
            moved=4 * rows * features,
            limit=16 * MIB,
        )[0]

    def summed(own, other):
        return call(
            lambda *refs: add_pack_kernel(images, *refs),
            [((2 * rows, half), bf16, pl.BlockSpec(memory_space=pltpu.VMEM))],
            [pl.BlockSpec(memory_space=pltpu.VMEM)] * 2,
            (own, other),
            flops=4 * small,
            moved=8 * rows * features,
            limit=16 * MIB,
        )[0]

    arrived = sent(send_slots)
    own_rows = unpacked(arrived)
    their_rows = swapped(own_rows)
    arrived = sent(send_grads)
    own_grads = unpacked(arrived)
    their_grads = swapped(own_grads)
    first_proj = w_in[0]
    second_proj = w_out[0]
    own_pre = dot(own_rows, first_proj, NN)
    own_hidden = jax.nn.gelu(own_pre).astype(bf16)
    their_pre = dot(their_rows, first_proj, NN)
    their_hidden = jax.nn.gelu(their_pre).astype(bf16)
    their_part = dot(their_hidden, second_proj, NN).astype(bf16)
    sums_out = swapped(their_part)

    def before_gelu(pre, grads):
        return jax.vjp(jax.nn.gelu, pre)[1](dot(grads, second_proj, NT))[0].astype(bf16)

    own_grad_pre = before_gelu(own_pre, own_grads)
    their_grad_pre = before_gelu(their_pre, their_grads)
    their_part = dot(their_grad_pre, first_proj, NT).astype(bf16)
    sums_in = swapped(their_part)
    own_part = dot(own_hidden, second_proj, NN)
    to_send = summed(own_part, sums_out)
    returned = sent(to_send)

    slot_rows = jnp.concatenate([own_rows, their_rows])
    grad_rows = jnp.concatenate([own_grads, their_grads])
    hidden = jnp.concatenate([own_hidden, their_hidden])
    grad_pre = jnp.concatenate([own_grad_pre, their_grad_pre])
    chips = lax.axis_size("dp") // 2
    low = lax.axis_index("dp") % 2
    second_part = dot(grad_rows, hidden, TN).astype(bf16).reshape(chips, -1, features)
    second_pieces = to_other_chips(second_part)
    first_part = dot(slot_rows, grad_pre, TN).astype(bf16).reshape(chips, 2, -1, features)
    own_part = dot(own_grad_pre, first_proj, NT)
    to_send = summed(own_part, sums_in)
    grad_back = sent(to_send)
    first_sent = after(piece_of(first_part, 1 - low, 1), sums_in)
    first_other = to_neighbour(first_sent)

    (combine_part,) = call(
        lambda *refs: combine_kernel(images, *refs),
        [((images, slot_count, count), f32, local_ref)],
        [far_ref] * 3,
        (returned, cotangent, combine),
        scratch=[
            pltpu.VMEM((2 * rows, half), bf16),
            stacked,
            pltpu.VMEM((images, slot_count, count), f32),
            pltpu.VMEM((rows, features), bf16),
            pltpu.SemaphoreType.DMA((images,)),
            pltpu.SemaphoreType.DMA((2,)),
        ],
        flops=10 * small,
        moved=2 * images * count * features,
    )
    grads, pair, sums = call(
        lambda *refs: logits_kernel(images, *refs),
        [
            ((rows, features), bf16, local_ref),
            ((images, 2 * slot_count + 16, count), bf16, local_ref),
            ((group * ROWS, LANES), f32, local_ref),
        ],
        [far_ref] * 8,
        (grad_back, slots, normed, logits, dispatch, combine_part, keys, gain),
        scratch=[
            pltpu.VMEM((2 * rows, half), bf16),
            pltpu.VMEM((rows, features), bf16),
            stacked,
        ]
        + [pltpu.VMEM((images, slot_count, count), f32)] * 3
        + [
            pltpu.VMEM((slot_count, features), bf16),
            pltpu.VMEM((1, features), f32),
            pltpu.VMEM((2 * slot_count, features), f32),
            pltpu.SemaphoreType.DMA((images,)),
            pltpu.SemaphoreType.DMA((7,)),
        ],
        flops=15 * small,
        moved=2 * images * count * features,
    )
    mine = lax.all_to_all(sums.reshape(group, ROWS, LANES), "expert", 0, 0, tiled=True)
    mine = jnp.sum(mine, axis=0)
    mine_two = from_everyone(mine, ("dp", "tensor"))
    first_other = after(first_other, mine)
    first_pieces = list(rotated_sum(first_part, first_other))
    size = lax.axis_size("dp")
    first_pieces = first_pieces[:1] + [
        lax.ppermute(first_pieces[k], "dp", chip_pairs(k, size)) for k in range(1, chips)
    ]
    second_pieces = after(second_pieces, sums)
    second_kept, second_sent = split_sum(second_part, second_pieces)
    second_other = to_neighbour(second_sent)
    mine = jnp.sum(mine_two, axis=0)
    total = from_everyone(mine, "expert").reshape(-1, LANES)
    blocks = features // LANES
    keys_sum = total[: slot_count * blocks].reshape(blocks, slot_count, LANES)
    keys_sum = keys_sum.transpose(1, 0, 2).reshape(slot_count, features)
    gain_sum = total[slot_count * blocks :][:blocks].reshape(-1)
    gain_sum = gain_sum + jnp.sum(keys.astype(f32) * keys_sum, axis=0)

    (grad_tokens,) = call(
        tokens_kernel,
        [((images, count, features), bf16, tall)],
        [
            tall,
            tall,
            per_image(count, LANES),
            per_image(2 * slot_count + 16, count),
            thin,
            pl.BlockSpec((slot_count, features), lambda i: (i, 0)),
            whole(slot_count, features),
            whole(1, features),
        ],
        (normed, cotangent, inverse, pair, dispatch, grads, keys, gain),
        grid=images,
        scratch=[pltpu.VMEM((count, features + 2 * LANES), f32), pltpu.VMEM((1, features), f32)],
        flops=20 * small,
        moved=6 * images * count * features,
    )
    first_pieces = after(first_pieces, grad_tokens)
    grad_first = added(first_pieces).astype(bf16)
    second_other = after(second_other, grad_tokens)
    grad_second = added([second_kept, second_other]).astype(bf16)
    return (
        grad_tokens,
        gain_sum / norm_gain,
        keys_sum.T,
        grad_first[None],
        grad_second.T[None],
    )


def solution(mesh):
    placed = (
        P(("dp", "expert", "tensor"), None, None),
        P(("dp", "expert", "tensor"), None, None),
        P(),
        P(),
        P("expert", None, "tensor"),
        P("expert", "tensor", None),
    )
    return jax.shard_map(
        local,
        mesh=mesh,
        in_specs=placed,
        out_specs=(
            P(("dp", "expert", "tensor"), None, None),
            P(),
            P(),
            P("expert", "dp", "tensor"),
            P("expert", "tensor", "dp"),
        ),
        check_vma=False,
    )
```

```python
import jax
import jax.numpy as jnp
from jax import lax
from jax.experimental import pallas as pl
from jax.experimental.pallas import tpu as pltpu
from jax.sharding import PartitionSpec as P


SLOT_PER = 2


EPSILON = 1e-06


ROWS = 24
LANES = 128
CHUNK = 16
MIB = 1024 * 1024


def dot(left, right, dims):
    return lax.dot_general(left, right, (dims, ((), ())), preferred_element_type=jnp.float32)


NN = ((1,), (0,))
NT = ((1,), (1,))
TN = ((0,), (0,))


def from_everyone(shard, axis):
    devices = lax.axis_size(axis)
    return lax.all_to_all(
        jnp.broadcast_to(shard[None], (devices, *shard.shape)), axis, 0, 0, tiled=True
    )


def swapped(value):
    return lax.ppermute(value, "tensor", [(0, 1), (1, 0)])


def call(kernel, outs, ins, args, grid=None, scratch=(), flops=0, moved=0, limit=None):
    specs = {} if grid is None else {"grid": (grid,)}
    return pl.pallas_call(
        kernel,
        out_shape=[jax.ShapeDtypeStruct(s, d) for s, d, _ in outs],
        in_specs=list(ins),
        out_specs=[spec for _, _, spec in outs],
        scratch_shapes=list(scratch),
        compiler_params=pltpu.CompilerParams(vmem_limit_bytes=limit),
        cost_estimate=pl.CostEstimate(flops=flops, bytes_accessed=moved, transcendentals=0),
        **specs,
    )(*args)


def per_image(rows, cols):
    return pl.BlockSpec((1, rows, cols), lambda i: (i, 0, 0))


def whole(*shape):
    return pl.BlockSpec(shape, lambda i: (0,) * len(shape))


def packed_place(place, images):
    block = images * SLOT_PER
    place = place.astype(jnp.float32)
    expert = jnp.floor((place + 0.5) * (1.0 / (2 * block)))
    rest = place - expert * (2 * block)
    half = jnp.floor((rest + 0.5) * (1.0 / block))
    rest = rest - half * block
    image = jnp.floor((rest + 0.5) * (1.0 / SLOT_PER))
    return expert, half, image, rest - image * SLOT_PER


def selection(rows, images, half, by_image, packed_first):
    shape = (2 * rows, rows) if packed_first else (rows, 2 * rows)
    along = 0 if packed_first else 1
    thin = (2 * rows, 1) if packed_first else (1, 2 * rows)
    expert, part, image, slot = packed_place(lax.broadcasted_iota(jnp.int32, thin, along), images)
    if by_image:
        target = image * (rows // images) + expert * SLOT_PER + slot
    else:
        target = expert * (images * SLOT_PER) + image * SLOT_PER + slot
    target = jnp.where(part == half, target, -1.0)
    plain = lax.broadcasted_iota(jnp.int32, shape, 1 - along).astype(jnp.float32)
    return jnp.where(plain == target, 1.0, 0.0).astype(jnp.bfloat16)


def pack(value, images, by_image):
    rows, cols = value.shape
    total = 0.0
    for half in range(2):
        pick = selection(rows, images, half, by_image, True)
        total = total + dot(pick, value[:, half * (cols // 2) : (half + 1) * (cols // 2)], NN)
    return total.astype(jnp.bfloat16)


def unpack_into(out_ref, value, images, by_image):
    rows, cols = out_ref.shape
    for half in range(2):
        pick = selection(rows, images, half, by_image, False)
        out_ref[:, half * (cols // 2) : (half + 1) * (cols // 2)] = dot(pick, value, NN).astype(
            jnp.bfloat16
        )


def parts(wide, count):
    pieces = []
    for _ in range(count):
        piece = wide.astype(jnp.bfloat16)
        pieces.append(piece)
        wide = wide - piece.astype(jnp.float32)
    return pieces


def over_chunks(count, body):
    def group(g, carry):
        for part in range(4):
            body(pl.ds(pl.multiple_of((g * 4 + part) * CHUNK, CHUNK), CHUNK))
        return carry

    lax.fori_loop(0, count // (4 * CHUNK), group, 0)


def lane_blocks(features):
    return [slice(k * LANES, (k + 1) * LANES) for k in range(features // LANES)]


def softmax(logits, axis):
    exps = jnp.exp(logits - jnp.max(logits, axis=axis, keepdims=True))
    return exps / jnp.sum(exps, axis=axis, keepdims=True)


def started(copies):
    for copy in copies:
        copy.start()
    return copies


def copies_of(sources, targets, sems):
    return [
        pltpu.make_async_copy(source, target, sems.at[i])
        for i, (source, target) in enumerate(zip(sources, targets))
    ]


def forward_kernel(images, *refs):
    inputs, outputs, held = refs[:3], refs[3:10], refs[10:]
    tok, flat, keys, send, slots, normed, inverse, logs, disp, comb, mean, squares, gain = held[:13]
    in_sems, small_sems, exit_sems, out_sems = held[13:]
    count, features = tok.shape[1:]
    slot_count = keys.shape[0]
    tokens_in = [inputs[0].at[i] for i in range(images)]
    arrivals = started(copies_of(tokens_in, [tok.at[i] for i in range(images)], in_sems))
    small_in = started(copies_of(inputs[1:], [flat, keys], small_sems))
    exits = copies_of(
        [normed.at[i] for i in range(images)], [outputs[2].at[i] for i in range(images)], exit_sems
    )
    results = copies_of(
        [send, slots, inverse, logs, disp, comb], outputs[:2] + outputs[3:], out_sems
    )
    ones = jnp.ones((features, LANES), jnp.bfloat16)
    for i in range(images):
        arrivals[i].wait()
        mean[i] = dot(tok[i], ones, NN) * (1.0 / features)

        def square(rows):
            middle = mean[i, rows, :]
            total = jnp.zeros_like(middle)
            for at in lane_blocks(features):
                centred = tok[i, rows, at].astype(jnp.float32) - middle
                total = total + centred * centred
            squares[i, rows, :] = total

        over_chunks(count, square)
    for i in range(images):
        spread = 0.0
        for piece in parts(squares[i], 3):
            spread = spread + dot(piece, ones[:LANES], NN)
        inverse[i] = lax.rsqrt(spread * (1.0 / features) + EPSILON)
    results[2].start()
    for copy in small_in:
        copy.wait()
    gain[...] = flat[...].reshape(1, features)
    for i in range(images):

        def norm(rows):
            middle = mean[i, rows, :]
            scale = inverse[i, rows, :]
            for at in lane_blocks(features):
                centred = tok[i, rows, at].astype(jnp.float32) - middle
                normed[i, rows, at] = (centred * scale * gain[0:1, at]).astype(jnp.bfloat16)

        over_chunks(count, norm)
        exits[i].start()
    for i in range(images):
        logs[i] = dot(keys[...], normed[i], NT)
    results[3].start()
    for i in range(images):
        disp[i] = softmax(logs[i], 1)
        comb[i] = softmax(logs[i], 0)
    results[4].start()
    results[5].start()
    for i in range(images):
        values = dot(disp[i].astype(jnp.bfloat16), normed[i], NN)
        slots[i * slot_count : (i + 1) * slot_count, :] = values.astype(jnp.bfloat16)
    results[1].start()
    send[...] = pack(slots[...], images, True)
    results[0].start()
    for copy in exits + results:
        copy.wait()


def grads_kernel(images, cot, comb, send, slots):
    i = pl.program_id(0)
    count = comb.shape[1]
    values = dot(comb[0].astype(jnp.bfloat16), cot[0], NN)
    slots[pl.ds(pl.multiple_of(i * count, count), count), :] = values.astype(jnp.bfloat16)

    @pl.when(i == images - 1)
    def _():
        send[...] = pack(slots[...], images, True)


def unpack_kernel(images, value, out):
    unpack_into(out, value[...], images, False)


def add_pack_kernel(images, own, other, out):
    total = (own[...] + other[...].astype(jnp.float32)).astype(jnp.bfloat16)
    out[...] = pack(total, images, False)


def combine_kernel(images, far_back, hbm, far_comb, out, back, cot, comb, slots, sems, small_sems):
    smalls = started(copies_of([far_back, far_comb], [back, comb], small_sems))
    per = [hbm.at[i] for i in range(images)]
    arrivals = started(copies_of(per, [cot.at[i] for i in range(images)], sems))
    for copy in smalls:
        copy.wait()
    unpack_into(slots, back[...], images, True)
    count = comb.shape[1]
    for copy in arrivals:
        copy.wait()
    grad_all = [dot(slots[i * count : (i + 1) * count, :], cot[i], NT) for i in range(images)]
    for i in range(images):
        grad = grad_all[i]
        weight = comb[i]
        out[i] = weight * (grad - jnp.sum(weight * grad, axis=0, keepdims=True))


def logits_kernel(images, *refs):
    inputs, (grads, pair, sums), held = refs[:8], refs[8:11], refs[11:]
    back, slots, normed, logs, disp, part, keys, gain, total, sems, small_sems = held
    targets = [back, logs, disp, part, keys, gain, slots]
    sources = [inputs[0]] + list(inputs[3:]) + [inputs[1]]
    smalls = started(copies_of(sources, targets, small_sems))
    per = [inputs[2].at[i] for i in range(images)]
    arrivals = started(copies_of(per, [normed.at[i] for i in range(images)], sems))
    smalls[0].wait()
    unpack_into(grads, back[...], images, True)
    for copy in smalls[1:]:
        copy.wait()
    count = disp.shape[1]
    tokens = normed.shape[1]
    share = 1.0 / normed.shape[2]
    keys_share = jnp.sum(keys[...].astype(jnp.float32) * gain[...], axis=1, keepdims=True)
    place = lax.broadcasted_iota(jnp.int32, (16, tokens), 0)
    grad_all = []
    for copy in arrivals:
        copy.wait()
    for i in range(images):
        mine = grads[i * count : (i + 1) * count, :]
        grad_all.append(dot(mine, normed[i], NT))
    updates = []
    for i in range(images):
        mine = grads[i * count : (i + 1) * count, :]
        grad = grad_all[i]
        weight = disp[i]
        wide = weight * (grad - jnp.sum(weight * grad, axis=1, keepdims=True)) + part[i]
        high, rest = parts(wide, 2)
        pair[i, :count, :] = high
        pair[i, count : 2 * count, :] = rest
        updates.append(jnp.concatenate([high, rest], axis=0))
        used = high.astype(jnp.float32) + rest.astype(jnp.float32)
        spread = weight.astype(jnp.bfloat16).astype(jnp.float32)
        mine_share = jnp.sum(mine.astype(jnp.float32) * gain[...], axis=1, keepdims=True)
        first = jnp.sum(spread * mine_share + used * keys_share, axis=0, keepdims=True) * share
        second = jnp.sum(spread * grad + used * logs[i], axis=0, keepdims=True) * share
        rows = jnp.zeros((16, tokens), jnp.float32)
        for k, row in enumerate(parts(first, 2) + parts(second, 2)):
            rows = jnp.where(place == k, row.astype(jnp.float32), rows)
        pair[i, 2 * count :, :] = rows.astype(jnp.bfloat16)
    flat = normed[...].reshape(images * tokens, normed.shape[2])
    total[...] = dot(jnp.concatenate(updates, axis=1), flat, NN)
    product = grads[...].astype(jnp.float32) * slots[...].astype(jnp.float32)
    moved = jnp.sum(product, axis=0, keepdims=True)
    blocks = moved.shape[1] // LANES
    sums[blocks * count :, :] = jnp.zeros((sums.shape[0] - blocks * count, LANES), jnp.float32)
    for k, at in enumerate(lane_blocks(moved.shape[1])):
        sums[k * count : (k + 1) * count, :] = total[:count, at] + total[count:, at]
        sums[blocks * count + k : blocks * count + k + 1, :] = moved[:, at]


def tokens_kernel(normed, cot, inverse, pair, disp, grads, keys, gain, out, wide, inside):
    count, features = normed.shape[1:]
    weights = jnp.concatenate([disp[0].astype(jnp.bfloat16), pair[0]], axis=0)
    extra = weights.shape[0] - 3 * keys.shape[0]
    values = jnp.concatenate(
        [grads[...], keys[...], keys[...], jnp.zeros((extra, features), jnp.bfloat16)], axis=0
    )
    inside[...] = 1.0 / gain[...]
    wide[:, :features] = dot(weights, values, TN)
    row = lax.broadcasted_iota(jnp.int32, (extra, 2 * LANES), 0)
    col = lax.broadcasted_iota(jnp.int32, (extra, 2 * LANES), 1)
    pick = jnp.where((row < 4) & ((row < 2) == (col < LANES)), 1.0, 0.0).astype(jnp.bfloat16)
    wide[:, features:] = dot(pair[0, 2 * keys.shape[0] :, :], pick, TN)

    def norm(rows):
        first = wide[rows, features : features + LANES]
        second = wide[rows, features + LANES :]
        scale = inverse[0, rows, :]
        for at in lane_blocks(features):
            scaled = normed[0, rows, at].astype(jnp.float32) * inside[:, at]
            result = scale * (wide[rows, at] * gain[:, at] - first - scaled * second)
            out[0, rows, at] = (cot[0, rows, at].astype(jnp.float32) + result).astype(jnp.bfloat16)

    over_chunks(count, norm)


def after(value, *others):
    return lax.optimization_barrier((value, others))[0]


def piece_of(pieces, index, axis=0):
    return lax.dynamic_index_in_dim(pieces, index, axis, keepdims=False)


def chip_pairs(step, size):
    return [(i, (i + 2 * step) % size) for i in range(size)]


def rotated_sum_kernel(where, far_part, far_other, *refs):
    chips = far_other.shape[0]
    outs, (part, other, sems) = refs[:chips], refs[chips:]
    order = [lax.rem(where[0] + k, chips) for k in range(chips)]
    copies = copies_of(
        [far_part.at[at, where[1]] for at in order] + [far_other.at[at] for at in order],
        [part.at[k] for k in range(chips)] + [other.at[k] for k in range(chips)],
        sems,
    )
    started(copies)
    for k in range(chips):
        copies[k].wait()
        copies[chips + k].wait()
        outs[k][...] = added([part[k], other[k]]).astype(jnp.bfloat16)


def rotated_sum(part, other):
    chips, _, rows, cols = part.shape
    index = lax.axis_index("dp")
    where = jnp.stack([index // 2, index % 2]).astype(jnp.int32)
    return call(
        rotated_sum_kernel,
        [((rows, cols), jnp.bfloat16, pl.BlockSpec(memory_space=pltpu.VMEM))] * chips,
        [pl.BlockSpec(memory_space=pltpu.SMEM)] + [pl.BlockSpec(memory_space=pl.ANY)] * 2,
        (where, part, other),
        scratch=[pltpu.VMEM((chips, rows, cols), jnp.bfloat16)] * 2
        + [pltpu.SemaphoreType.DMA((2 * chips,))],
        flops=100 * rows * cols * chips,
        moved=6 * rows * cols * chips,
    )


def split_sum_kernel(where, far_part, *refs):
    arrived, (kept, sent, held, sems) = refs[:-4], refs[-4:]
    chips = len(arrived) + 1
    rows = kept.shape[0]
    sources = [far_part.at[where[0]]] + list(arrived)
    copies = started(copies_of(sources, [held.at[k] for k in range(chips)], sems))
    for copy in copies:
        copy.wait()

    def total(low):
        at = pl.ds(pl.multiple_of(low * rows, CHUNK), rows)
        return added([held[k, at, :] for k in range(chips)])

    kept[...] = total(where[1])
    sent[...] = total(1 - where[1]).astype(jnp.bfloat16)


def split_sum(part, arrived):
    chips, rows, cols = part.shape
    index = lax.axis_index("dp")
    where = jnp.stack([index // 2, index % 2]).astype(jnp.int32)
    local_ref = pl.BlockSpec(memory_space=pltpu.VMEM)
    return call(
        split_sum_kernel,
        [((rows // 2, cols), jnp.float32, local_ref), ((rows // 2, cols), jnp.bfloat16, local_ref)],
        [pl.BlockSpec(memory_space=pltpu.SMEM)] + [pl.BlockSpec(memory_space=pl.ANY)] * chips,
        (where, part, *arrived),
        scratch=[pltpu.VMEM((chips, rows, cols), jnp.bfloat16), pltpu.SemaphoreType.DMA((chips,))],
        flops=100 * rows * cols * chips,
        moved=2 * rows * cols * chips,
    )


def to_other_chips(pieces):
    size = lax.axis_size("dp")
    chips = size // 2
    at = lax.axis_index("dp") // 2
    arrived = [
        lax.ppermute(piece_of(pieces, (at + step) % chips), "dp", chip_pairs(step, size))
        for step in range(1, chips)
    ]
    return arrived


def to_neighbour(value):
    return lax.ppermute(value, "dp", [(i, i ^ 1) for i in range(lax.axis_size("dp"))])


def added(pieces):
    total = pieces[0].astype(jnp.float32)
    for piece in pieces[1:]:
        total = total + piece.astype(jnp.float32)
    return total


def local(tokens, cotangent, norm_gain, slot_keys, w_in, w_out):
    images, count, features = tokens.shape
    slot_count = slot_keys.shape[1]
    rows = images * slot_count
    group = slot_count // SLOT_PER
    half = features // 2
    bf16, f32 = jnp.bfloat16, jnp.float32
    keys = slot_keys.T
    gain = norm_gain.reshape(1, features)
    tall = per_image(count, features)
    thin = per_image(slot_count, count)
    packed = whole(2 * rows, half)
    small = 2 * rows * features * count

    def sent(value):
        shaped = value.reshape(group, -1, half)
        return lax.all_to_all(shaped, "expert", 0, 0, tiled=True).reshape(2 * rows, half)

    local_ref = pl.BlockSpec(memory_space=pltpu.VMEM)
    far_ref = pl.BlockSpec(memory_space=pl.ANY)
    stacked = pltpu.VMEM((images, count, features), bf16)
    kept = [
        ((2 * rows, half), bf16),
        ((rows, features), bf16),
        ((images, count, features), bf16),
        ((images, count, LANES), f32),
        ((images, slot_count, count), f32),
        ((images, slot_count, count), f32),
        ((images, slot_count, count), f32),
    ]
    send_slots, slots, normed, inverse, logits, dispatch, combine = call(
        lambda *refs: forward_kernel(images, *refs),
        [(shape, kind, far_ref) for shape, kind in kept],
        [far_ref] * 3,
        (tokens, norm_gain, keys),
        scratch=[stacked, pltpu.VMEM((features,), f32), pltpu.VMEM((slot_count, features), bf16)]
        + [pltpu.VMEM(shape, kind) for shape, kind in kept]
        + [pltpu.VMEM((images, count, LANES), f32)] * 2
        + [pltpu.VMEM((1, features), f32)]
        + [pltpu.SemaphoreType.DMA((n,)) for n in (images, 2, images, 6)],
        flops=20 * small,
        moved=4 * images * count * features,
    )
    (send_grads,) = call(
        lambda *refs: grads_kernel(images, *refs),
        [((2 * rows, half), bf16, packed)],
        [tall, thin],
        (cotangent, combine),
        grid=images,
        scratch=[pltpu.VMEM((rows, features), bf16)],
        flops=10 * small,
        moved=2 * images * count * features,
    )

    def unpacked(value):
        return call(
            lambda *refs: unpack_kernel(images, *refs),
            [((rows, features), bf16, pl.BlockSpec(memory_space=pltpu.VMEM))],
            [pl.BlockSpec(memory_space=pltpu.VMEM)],
            (value,),
            flops=4 * small,
            moved=4 * rows * features,
            limit=16 * MIB,
        )[0]

    def summed(own, other):
        return call(
            lambda *refs: add_pack_kernel(images, *refs),
            [((2 * rows, half), bf16, pl.BlockSpec(memory_space=pltpu.VMEM))],
            [pl.BlockSpec(memory_space=pltpu.VMEM)] * 2,
            (own, other),
            flops=4 * small,
            moved=8 * rows * features,
            limit=16 * MIB,
        )[0]

    arrived = sent(send_slots)
    own_rows = unpacked(arrived)
    their_rows = swapped(own_rows)
    arrived = sent(send_grads)
    own_grads = unpacked(arrived)
    their_grads = swapped(own_grads)
    first_proj = w_in[0]
    second_proj = w_out[0]
    own_pre = dot(own_rows, first_proj, NN)
    own_hidden = jax.nn.gelu(own_pre).astype(bf16)
    their_pre = dot(their_rows, first_proj, NN)
    their_hidden = jax.nn.gelu(their_pre).astype(bf16)
    their_part = dot(their_hidden, second_proj, NN).astype(bf16)
    sums_out = swapped(their_part)

    def before_gelu(pre, grads):
        return jax.vjp(jax.nn.gelu, pre)[1](dot(grads, second_proj, NT))[0].astype(bf16)

    own_grad_pre = before_gelu(own_pre, own_grads)
    their_grad_pre = before_gelu(their_pre, their_grads)
    their_part = dot(their_grad_pre, first_proj, NT).astype(bf16)
    sums_in = swapped(their_part)
    own_part = dot(own_hidden, second_proj, NN)
    to_send = summed(own_part, sums_out)
    returned = sent(to_send)

    slot_rows = jnp.concatenate([own_rows, their_rows])
    grad_rows = jnp.concatenate([own_grads, their_grads])
    hidden = jnp.concatenate([own_hidden, their_hidden])
    grad_pre = jnp.concatenate([own_grad_pre, their_grad_pre])
    chips = lax.axis_size("dp") // 2
    low = lax.axis_index("dp") % 2
    second_part = dot(grad_rows, hidden, TN).astype(bf16).reshape(chips, -1, features)
    second_pieces = to_other_chips(second_part)
    first_part = dot(slot_rows, grad_pre, TN).astype(bf16).reshape(chips, 2, -1, features)
    own_part = dot(own_grad_pre, first_proj, NT)
    to_send = summed(own_part, sums_in)
    grad_back = sent(to_send)
    first_sent = after(piece_of(first_part, 1 - low, 1), sums_in)
    first_other = to_neighbour(first_sent)

    (combine_part,) = call(
        lambda *refs: combine_kernel(images, *refs),
        [((images, slot_count, count), f32, local_ref)],
        [far_ref] * 3,
        (returned, cotangent, combine),
        scratch=[
            pltpu.VMEM((2 * rows, half), bf16),
            stacked,
            pltpu.VMEM((images, slot_count, count), f32),
            pltpu.VMEM((rows, features), bf16),
            pltpu.SemaphoreType.DMA((images,)),
            pltpu.SemaphoreType.DMA((2,)),
        ],
        flops=10 * small,
        moved=2 * images * count * features,
    )
    grads, pair, sums = call(
        lambda *refs: logits_kernel(images, *refs),
        [
            ((rows, features), bf16, local_ref),
            ((images, 2 * slot_count + 16, count), bf16, local_ref),
            ((group * ROWS, LANES), f32, local_ref),
        ],
        [far_ref] * 8,
        (grad_back, slots, normed, logits, dispatch, combine_part, keys, gain),
        scratch=[
            pltpu.VMEM((2 * rows, half), bf16),
            pltpu.VMEM((rows, features), bf16),
            stacked,
        ]
        + [pltpu.VMEM((images, slot_count, count), f32)] * 3
        + [
            pltpu.VMEM((slot_count, features), bf16),
            pltpu.VMEM((1, features), f32),
            pltpu.VMEM((2 * slot_count, features), f32),
            pltpu.SemaphoreType.DMA((images,)),
            pltpu.SemaphoreType.DMA((7,)),
        ],
        flops=15 * small,
        moved=2 * images * count * features,
    )
    mine = lax.all_to_all(sums.reshape(group, ROWS, LANES), "expert", 0, 0, tiled=True)
    mine = jnp.sum(mine, axis=0)
    mine_two = from_everyone(mine, ("dp", "tensor"))
    first_other = after(first_other, mine)
    first_pieces = list(rotated_sum(first_part, first_other))
    size = lax.axis_size("dp")
    first_pieces = first_pieces[:1] + [
        lax.ppermute(first_pieces[k], "dp", chip_pairs(k, size)) for k in range(1, chips)
    ]
    second_pieces = after(second_pieces, sums)
    second_kept, second_sent = split_sum(second_part, second_pieces)
    second_other = to_neighbour(second_sent)
    mine = jnp.sum(mine_two, axis=0)
    total = from_everyone(mine, "expert").reshape(-1, LANES)
    blocks = features // LANES
    keys_sum = total[: slot_count * blocks].reshape(blocks, slot_count, LANES)
    keys_sum = keys_sum.transpose(1, 0, 2).reshape(slot_count, features)
    gain_sum = total[slot_count * blocks :][:blocks].reshape(-1)
    gain_sum = gain_sum + jnp.sum(keys.astype(f32) * keys_sum, axis=0)

    (grad_tokens,) = call(
        tokens_kernel,
        [((images, count, features), bf16, tall)],
        [
            tall,
            tall,
            per_image(count, LANES),
            per_image(2 * slot_count + 16, count),
            thin,
            pl.BlockSpec((slot_count, features), lambda i: (i, 0)),
            whole(slot_count, features),
            whole(1, features),
        ],
        (normed, cotangent, inverse, pair, dispatch, grads, keys, gain),
        grid=images,
        scratch=[pltpu.VMEM((count, features + 2 * LANES), f32), pltpu.VMEM((1, features), f32)],
        flops=20 * small,
        moved=6 * images * count * features,
    )
    first_pieces = after(first_pieces, grad_tokens)
    grad_first = added(first_pieces).astype(bf16)
    second_other = after(second_other, grad_tokens)
    grad_second = added([second_kept, second_other]).astype(bf16)
    return (
        grad_tokens,
        gain_sum / norm_gain,
        keys_sum.T,
        grad_first[None],
        grad_second.T[None],
    )


def solution(mesh):
    placed = (
        P(("dp", "expert", "tensor"), None, None),
        P(("dp", "expert", "tensor"), None, None),
        P(),
        P(),
        P("expert", None, "tensor"),
        P("expert", "tensor", None),
    )
    return jax.shard_map(
        local,
        mesh=mesh,
        in_specs=placed,
        out_specs=(
            P(("dp", "expert", "tensor"), None, None),
            P(),
            P(),
            P("expert", "dp", "tensor"),
            P("expert", "tensor", "dp"),
        ),
        check_vma=False,
    )
```
